32 devices in a mesh: dom: 4 (over z), ens: 8 (over y, x, core).
Axes of the slice: x: 2, y: 2, z: 4, core: 2. Of those that a mesh axis runs over, the one named last changes fastest.
Arguments:
- ensemble: bfloat16 [128, 1024, 32, 73], P('ens', None, 'dom')
- w_in: bfloat16 [146, 256], replicated
- w_out: bfloat16 [256, 73], replicated
- obs_op: bfloat16 [73, 16], replicated
- obs_val: float32 [1024, 32, 16], P(None, 'dom')
- obs_wt: float32 [1024, 32, 16], P(None, 'dom')
Outputs:
- output: bfloat16 [128, 1024, 32, 73], P('ens', None, 'dom')
All inputs are finite; a program needn't handle non-finite values.
Results may differ from the reference program's by a relative error of at most 0.001.
Values are sent between devices in bfloat16 or wider.
A program may use at most 1 GiB of HBM per device.

```python
import jax
import jax.numpy as jnp
import numpy as np
from jax import lax

MEMBERS = 128
GRID_LAT = 1024
GRID_LON = 32
CHANNELS = 73
HIDDEN = 256
OBS_CH = 16
PATCH_SIDE = 8
LOC_RADIUS = 4
NS_STEPS = 20

WIN_COLS = PATCH_SIDE + 2 * LOC_RADIUS
WIN_OBS = PATCH_SIDE * WIN_COLS * OBS_CH


def setup_inputs(seed: int = 0) -> dict:
    key_list = jax.random.split(jax.random.key(seed), 8)
    base_field = jax.random.normal(key_list[0], (GRID_LAT, GRID_LON, CHANNELS), jnp.float32)
    spread = jax.random.normal(key_list[1], (MEMBERS, GRID_LAT, GRID_LON, CHANNELS), jnp.float32)
    ensemble = (0.7 * base_field[None] + 0.6 * spread).astype(jnp.bfloat16)
    w_state = jax.random.normal(key_list[2], (CHANNELS, HIDDEN), jnp.float32) * CHANNELS ** -0.5
    w_lap = jax.random.normal(key_list[3], (CHANNELS, HIDDEN), jnp.float32) * (20.0 * CHANNELS) ** -0.5
    w_in = jnp.concatenate([w_state, w_lap], axis=0).astype(jnp.bfloat16)
    w_out = (jax.random.normal(key_list[4], (HIDDEN, CHANNELS), jnp.float32) * (0.8 * HIDDEN ** -0.5)).astype(jnp.bfloat16)
    obs_op = (jax.random.normal(key_list[5], (CHANNELS, OBS_CH), jnp.float32) * CHANNELS ** -0.5).astype(jnp.bfloat16)
    obs_val = 0.9 * jax.random.normal(key_list[6], (GRID_LAT, GRID_LON, OBS_CH), jnp.float32)
    wt_scale = (MEMBERS - 1) / (0.5 * (MEMBERS ** 0.5 + WIN_OBS ** 0.5) ** 2)
    obs_wt = wt_scale * jax.random.uniform(key_list[7], (GRID_LAT, GRID_LON, OBS_CH), jnp.float32, 0.25, 1.75)
    return {'ensemble': ensemble, 'w_in': w_in, 'w_out': w_out, 'obs_op': obs_op, 'obs_val': obs_val, 'obs_wt': obs_wt}


def forecast_member(member, w_in, w_out):
    center = member.astype(jnp.float32)
    north_nb = jnp.concatenate([center[:1], center[:-1]], axis=0)
    south_nb = jnp.concatenate([center[1:], center[-1:]], axis=0)
    west_nb = jnp.roll(center, 1, axis=1)
    east_nb = jnp.roll(center, -1, axis=1)
    lap_bf = (north_nb + south_nb + west_nb + east_nb - 4.0 * center).astype(jnp.bfloat16)
    feat_rows = jnp.concatenate([member, lap_bf], axis=-1)
    feat_rows = feat_rows.reshape(GRID_LAT // PATCH_SIDE, PATCH_SIDE * GRID_LON, 2 * CHANNELS)

    def band_mlp(band_feats):
        hidden = jnp.dot(band_feats, w_in, preferred_element_type=jnp.float32)
        act_bf = jax.nn.gelu(hidden).astype(jnp.bfloat16)
        return jnp.dot(act_bf, w_out, preferred_element_type=jnp.float32)

    tendency = lax.map(band_mlp, feat_rows).reshape(GRID_LAT, GRID_LON, CHANNELS)
    return (center + tendency).astype(jnp.bfloat16)


def patch_update(xf_patch, yb_win, yo_win, wt_win):
    eye_mem = jnp.eye(MEMBERS, dtype=jnp.float32)
    x_mean = jnp.mean(xf_patch, axis=0)
    x_anom = xf_patch - x_mean
    y_mean = jnp.mean(yb_win, axis=0)
    y_anom = yb_win - y_mean
    weighted = y_anom * wt_win
    a_matrix = (MEMBERS - 1) * eye_mem + jnp.dot(weighted, y_anom.T)
    trace_a = jnp.trace(a_matrix)

    def ns_step(ns_carry, unused):
        y_mat, z_mat = ns_carry
        t_mat = 0.5 * (3.0 * eye_mem - jnp.dot(z_mat, y_mat))
        return (jnp.dot(y_mat, t_mat), jnp.dot(t_mat, z_mat)), None

    ns_out, unused_out = lax.scan(ns_step, (a_matrix / trace_a, eye_mem), None, length=NS_STEPS)
    s_root = ns_out[1] / jnp.sqrt(trace_a)
    p_ana = jnp.dot(s_root, s_root)
    w_mean = jnp.dot(p_ana, jnp.dot(weighted, yo_win - y_mean))
    t_full = (MEMBERS - 1) ** 0.5 * s_root + w_mean[:, None]
    return x_mean + jnp.einsum('kbc,ke->ebc', x_anom, t_full)


def analysis_band(xf_band, yo_band, wt_band, obs_op):
    n_patch = GRID_LON // PATCH_SIDE
    win_idx = (np.arange(n_patch)[:, None] * PATCH_SIDE - LOC_RADIUS + np.arange(WIN_COLS)[None, :]) % GRID_LON
    xf_f32 = xf_band.astype(jnp.float32)
    ens_obs = jnp.einsum('eync,co->eyno', xf_f32, obs_op.astype(jnp.float32))
    yb_win = jnp.moveaxis(ens_obs[:, :, win_idx, :], 2, 0).reshape(n_patch, MEMBERS, WIN_OBS)
    yo_win = jnp.moveaxis(yo_band[:, win_idx, :], 1, 0).reshape(n_patch, WIN_OBS)
    wt_win = jnp.moveaxis(wt_band[:, win_idx, :], 1, 0).reshape(n_patch, WIN_OBS)
    xf_patch = xf_f32.reshape(MEMBERS, PATCH_SIDE, n_patch, PATCH_SIDE, CHANNELS)
    xf_patch = jnp.transpose(xf_patch, (2, 0, 1, 3, 4)).reshape(n_patch, MEMBERS, PATCH_SIDE * PATCH_SIDE, CHANNELS)
    updated = jax.vmap(patch_update)(xf_patch, yb_win, yo_win, wt_win)
    updated = updated.reshape(n_patch, MEMBERS, PATCH_SIDE, PATCH_SIDE, CHANNELS)
    updated = jnp.transpose(updated, (1, 2, 0, 3, 4)).reshape(MEMBERS, PATCH_SIDE, GRID_LON, CHANNELS)
    return updated.astype(jnp.bfloat16)


def reference(ensemble, w_in, w_out, obs_op, obs_val, obs_wt):
    forecast = lax.map(lambda member: forecast_member(member, w_in, w_out), ensemble)
    n_band = GRID_LAT // PATCH_SIDE
    xf_bands = jnp.moveaxis(forecast.reshape(MEMBERS, n_band, PATCH_SIDE, GRID_LON, CHANNELS), 1, 0)
    yo_bands = obs_val.reshape(n_band, PATCH_SIDE, GRID_LON, OBS_CH)
    wt_bands = obs_wt.reshape(n_band, PATCH_SIDE, GRID_LON, OBS_CH)
    band_out = lax.map(lambda band_args: analysis_band(band_args[0], band_args[1], band_args[2], obs_op), (xf_bands, yo_bands, wt_bands))
    return jnp.moveaxis(band_out, 0, 1).reshape(MEMBERS, GRID_LAT, GRID_LON, CHANNELS)
```

```python
import functools
import math

import jax
import jax.numpy as jnp
from jax import lax
from jax.experimental import pallas as pl
from jax.experimental.pallas import tpu as pltpu
from jax.sharding import PartitionSpec as P

PATCH = 8
OBS = 16
NS_STEPS = 20
CH = 73
CP = 80
KP = 592
HID = 256
MEM = 128
MLOC = 16
LON = 8
PITCH = 24
YL = 32
LATC = 256
NCHUNK = 4
NB = 4
COLS = ((1, 2, 5, 6), (0, 3, 4, 7))

F32 = jnp.float32
BF16 = jnp.bfloat16
INTERPRET = False


def col_of(group, xi):
    a, b = COLS[0][xi], COLS[1][xi]
    if isinstance(group, int):
        return COLS[group][xi]
    return a + group * (b - a)


def lane_swap(tiles, lane):
    low = lane < 64
    even = (lane // 32) % 2 == 0
    t0, t1, t2, t3 = tiles
    a = jnp.where(low, t0, pltpu.roll(t2, 64, 1))
    b = jnp.where(low, pltpu.roll(t0, 64, 1), t2)
    c = jnp.where(low, t1, pltpu.roll(t3, 64, 1))
    d = jnp.where(low, pltpu.roll(t1, 64, 1), t3)
    u0 = jnp.where(even, a, pltpu.roll(c, 32, 1))
    u1 = jnp.where(even, pltpu.roll(a, 96, 1), c)
    u2 = jnp.where(even, b, pltpu.roll(d, 32, 1))
    u3 = jnp.where(even, pltpu.roll(b, 96, 1), d)
    return u0, u1, u2, u3


def edge_kernel(x_ref, w_ref, e_ref, s_ref):
    s_ref[:, CH * 8:, :] = jnp.zeros((2, CP * 8 - CH * 8, 128), F32)
    for m in range(x_ref.shape[0]):
        for c in range(CH):
            for l in range(2):
                s_ref[l, 8 * c:8 * c + 8, :] = x_ref[m, c, :, 128 * l:128 * l + 128].astype(F32)
        for l in range(2):
            for ref, x in ((w_ref, 0), (e_ref, 7)):
                ref[m, :, 128 * l:128 * l + 128] = s_ref.at[l][pl.ds(x, CP, stride=8), :].astype(BF16)


def edge_columns(xt, q):
    nm = 2
    return pl.pallas_call(
        edge_kernel,
        grid=(MLOC // nm,),
        in_specs=[pl.BlockSpec((nm, CH, LON, LATC), lambda i: (i, 0, 0, q))],
        out_specs=[pl.BlockSpec((nm, CP, LATC), lambda i: (i, 0, 0))] * 2,
        out_shape=[jax.ShapeDtypeStruct((MLOC, CP, LATC), BF16)] * 2,
        scratch_shapes=[pltpu.VMEM((2, CP * 8, 128), F32)],
        cost_estimate=pl.CostEstimate(flops=4_000_000_000, bytes_accessed=6_000_000, transcendentals=0),
        name="edge",
        interpret=INTERPRET,
    )(xt)


def forecast_kernel(groups, first, last, *refs):
    halo = 1 in groups
    if halo:
        xc_ref, xl_ref, xr_ref, wh_ref, eh_ref, w1_ref, w2_ref, o_ref, s_ref, r_ref = refs
    else:
        xc_ref, xl_ref, xr_ref, w1_ref, w2_ref, o_ref, s_ref, r_ref = refs
    m = pl.program_id(0)

    @pl.when(m == 0)
    def _():
        s_ref[:, CH * PITCH:, :] = jnp.zeros((4, (CP - CH) * PITCH, 128), F32)

    for c in range(CH):
        row = c * PITCH + 8
        s_ref[0, row:row + 8, :] = xl_ref[0, c, :, :].astype(F32)
        s_ref[1, row:row + 8, :] = xc_ref[0, c, :, 0:128].astype(F32)
        s_ref[2, row:row + 8, :] = xc_ref[0, c, :, 128:256].astype(F32)
        s_ref[3, row:row + 8, :] = xr_ref[0, c, :, :].astype(F32)
    if halo:
        for l in range(2):
            s_ref.at[1 + l][pl.ds(7, CP, stride=PITCH), :] = wh_ref[0, :, 128 * l:128 * l + 128].astype(F32)
            s_ref.at[1 + l][pl.ds(16, CP, stride=PITCH), :] = eh_ref[0, :, 128 * l:128 * l + 128].astype(F32)

    lane = lax.broadcasted_iota(jnp.int32, (16, 128), 1)
    w1 = w1_ref[...]
    w2 = w2_ref[...]

    def column(gi, xi, x):
        feat_x, feat_l = [], []
        for cb in range(CP // 16):
            def slab(l, dx):
                return s_ref.at[l][pl.ds(8 + x + dx + cb * 16 * PITCH, 16, stride=PITCH), :]
            left, c0, c1, right = slab(0, 0), slab(1, 0), slab(2, 0), slab(3, 0)
            c0_n, c1_n = pltpu.roll(c0, 1, 1), pltpu.roll(c1, 1, 1)
            c0_s, c1_s = pltpu.roll(c0, 127, 1), pltpu.roll(c1, 127, 1)
            north0 = jnp.where(lane == 0, c0 if first else pltpu.roll(left, 1, 1), c0_n)
            north1 = jnp.where(lane == 0, c0_n, c1_n)
            south0 = jnp.where(lane == 127, c1_s, c0_s)
            south1 = jnp.where(lane == 127, c1 if last else pltpu.roll(right, 127, 1), c1_s)
            lap0 = north0 + south0 + slab(1, -1) + slab(1, 1) - 4.0 * c0
            lap1 = north1 + south1 + slab(2, -1) + slab(2, 1) - 4.0 * c1
            feat_x.append(jnp.concatenate([c0.astype(BF16), c1.astype(BF16)], axis=1))
            feat_l.append(jnp.concatenate([lap0.astype(BF16), lap1.astype(BF16)], axis=1))
        feats = jnp.concatenate(feat_x + feat_l, axis=0)
        hid = jnp.dot(w1, feats, preferred_element_type=F32)
        inner = hid * (math.sqrt(2.0 / math.pi) + (0.044715 * math.sqrt(2.0 / math.pi)) * (hid * hid))
        half = 0.5 * hid
        act = (half + half * jnp.tanh(inner)).astype(BF16)
        tend = jnp.dot(w2, act, preferred_element_type=F32)
        for l in range(2):
            center = s_ref.at[1 + l][pl.ds(8 + x, CP, stride=PITCH), :]
            r_ref.at[gi * 4 + xi, l][pl.ds(m, CP, stride=PITCH), :] = center + tend[:, 128 * l:128 * l + 128]

    if len(groups) == 1:
        for xi in range(4):
            column(0, xi, col_of(groups[0], xi))
    else:
        def body(gi, carry):
            for xi in range(4):
                column(gi, xi, col_of(gi, xi))
            return carry
        lax.fori_loop(0, 2, body, 0)

    @pl.when(m == MLOC - 1)
    def _():
        def body(c, carry):
            row = pl.multiple_of(c * PITCH, 8)
            for gi in range(len(groups)):
                for l in range(2):
                    tiles = [r_ref[gi * 4 + xi, l, pl.ds(row, 16), :] for xi in range(4)]
                    for j, tile in enumerate(lane_swap(tiles, lane)):
                        o_ref[4 * l + j, gi, c, :, :] = tile.astype(BF16)
            return carry
        lax.fori_loop(0, CH, body, 0)


def forecast(xt, q, groups, halos, w1t, w2t):
    ng = len(groups)
    first, last = q == 0, q == NCHUNK - 1
    lt, rt = max(2 * q - 1, 0), min(2 * q + 2, 2 * NCHUNK - 1)
    specs = [
        pl.BlockSpec((1, CH, LON, LATC), lambda m: (m, 0, 0, q)),
        pl.BlockSpec((1, CH, LON, 128), lambda m: (m, 0, 0, lt)),
        pl.BlockSpec((1, CH, LON, 128), lambda m: (m, 0, 0, rt)),
    ]
    args = [xt, xt, xt]
    if 1 in groups:
        specs += [pl.BlockSpec((1, CP, LATC), lambda m: (m, 0, 0))] * 2
        args += list(halos)
    specs += [pl.BlockSpec(w1t.shape, lambda m: (0, 0)), pl.BlockSpec(w2t.shape, lambda m: (0, 0))]
    return pl.pallas_call(
        functools.partial(forecast_kernel, groups, first, last),
        grid=(MLOC,),
        in_specs=specs,
        out_specs=pl.BlockSpec((8, ng, CH, 16, 128), lambda m: (0, 0, 0, 0, 0)),
        out_shape=jax.ShapeDtypeStruct((8, ng, CH, 16, 128), BF16),
        scratch_shapes=[
            pltpu.VMEM((4, CP * PITCH, 128), F32),
            pltpu.VMEM((ng * 4, 2, CP * PITCH, 128), F32),
        ],
        cost_estimate=pl.CostEstimate(flops=8_000_000_000 * ng, bytes_accessed=10_000_000, transcendentals=0),
        name="forecast",
        interpret=INTERPRET,
    )(*args, w1t, w2t)


def split3(val):
    p1 = val.astype(BF16)
    rest = val - p1.astype(F32)
    p2 = rest.astype(BF16)
    p3 = (rest - p2.astype(F32)).astype(BF16)
    return p1, p2, p3


def gram_kernel(n_in, *refs):
    x_refs = refs[:n_in]
    hk_ref, yo_ref, wt_ref, xt_ref, gl_ref, gr_ref = refs[n_in:]

    def source(g):
        return (x_refs[g], 0) if n_in == 2 else (x_refs[0], g)

    def turned(g, c):
        ref, gi = source(g)
        cols = jnp.concatenate([ref[src, gi, c, :, :] for src in range(8)], axis=0)
        return cols.astype(F32).T

    for g in range(2):
        def pair(cp, carry, g=g):
            top, low = turned(g, 2 * cp), turned(g, 2 * cp + 1)
            row = pl.multiple_of(cp * 16, 16)
            for t in range(16):
                both = jnp.concatenate([top[8 * t:8 * t + 8], low[8 * t:8 * t + 8]], axis=0)
                xt_ref[g * 16 + t, pl.ds(row, 16), :] = both.astype(BF16)
            return carry
        lax.fori_loop(0, CH // 2, pair, 0)
        top = turned(g, CH - 1)
        for t in range(16):
            both = jnp.concatenate([top[8 * t:8 * t + 8], jnp.zeros((8, 128), F32)], axis=0)
            xt_ref[g * 16 + t, KP - 16:KP, :] = both.astype(BF16)

    hk = hk_ref[...]
    for half, out_ref in ((0, gl_ref), (1, gr_ref)):
        def patch_pair(bp, carry, half=half, out_ref=out_ref):
            gram = [None, None]
            innov = [None, None]
            for g in range(2):
                for x2 in range(2):
                    base = g * 16 + (half * 2 + x2) * 4 + bp * 2
                    rhs = jnp.concatenate([xt_ref[base], xt_ref[base + 1]], axis=1)
                    yb = jnp.dot(hk, rhs, preferred_element_type=F32)
                    for i in range(2):
                        ybt = yb[:, 128 * i:128 * i + 128].T
                        mean = jnp.sum(ybt, axis=0, keepdims=True) * (1.0 / MEM)
                        anom = ybt - mean
                        wrow = wt_ref[pl.ds(base + i, 1), :]
                        yrow = yo_ref[pl.ds(base + i, 1), :]
                        cm = anom * wrow
                        inn = cm * (yrow - mean)
                        c1, c2, c3 = split3(cm)
                        p1, p2, p3 = split3(anom)
                        lhs = jnp.concatenate([c3, c1, c2, c2, c1, c1], axis=1)
                        rh = jnp.concatenate([p1, p3, p2, p1, p2, p1], axis=1)
                        part = lax.dot_general(lhs, rh, (((1,), (1,)), ((), ())), preferred_element_type=F32)
                        gram[i] = part if gram[i] is None else gram[i] + part
                        innov[i] = inn if innov[i] is None else innov[i] + inn
            for i in range(2):
                b = bp * 2 + i
                out_ref[b, 0:128, :] = gram[i]
                row = jnp.sum(innov[i].T, axis=0, keepdims=True)
                out_ref[b, 128:136, :] = jnp.broadcast_to(row, (8, 128))
            return carry
        lax.fori_loop(0, NB // 2, patch_pair, 0)


def gram(arrived, hk, yo, wt):
    vm = pl.BlockSpec(memory_space=pltpu.VMEM)
    n_in = len(arrived)
    return pl.pallas_call(
        functools.partial(gram_kernel, n_in),
        in_specs=[vm] * (n_in + 3),
        out_specs=[vm] * 3,
        out_shape=[
            jax.ShapeDtypeStruct((32, KP, 128), BF16),
            jax.ShapeDtypeStruct((NB, 136, 128), F32),
            jax.ShapeDtypeStruct((NB, 136, 128), F32),
        ],
        cost_estimate=pl.CostEstimate(flops=8_000_000_000, bytes_accessed=10_000_000, transcendentals=0),
        name="gram",
        interpret=INTERPRET,
    )(*arrived, hk, yo, wt)


def lhs_of(parts):
    p1, p2, p3 = parts
    return jnp.concatenate([p1, p2], axis=1), jnp.concatenate([p1, p3], axis=1)


def rhs_of(parts):
    p1, p2, p3 = parts
    top = jnp.concatenate([p1, p2], axis=1)
    return jnp.concatenate([top, top], axis=0), jnp.concatenate([p3, p1], axis=0)


def mm(lhs, rhs):
    main = jnp.dot(lhs[0], rhs[0], preferred_element_type=F32)
    tail = jnp.dot(lhs[1], rhs[1], preferred_element_type=F32)
    return main[:, :128] + (main[:, 128:] + tail)


def update_kernel(gl_ref, gr_ref, gw_ref, ge_ref, xt_ref, o_ref, y_ref, z_ref, t_ref, u_ref):
    rows = lax.broadcasted_iota(jnp.int32, (128, 128), 0)
    cols = lax.broadcasted_iota(jnp.int32, (128, 128), 1)
    eye = jnp.where(rows == cols, 1.0, 0.0).astype(F32)
    traces = []
    innovs = []
    for b in range(NB):
        full = (gw_ref[b] + gl_ref[b]) + (gr_ref[b] + ge_ref[b])
        a_mat = full[0:128] + (MEM - 1.0) * eye
        diag = jnp.sum(a_mat * eye, axis=0, keepdims=True)
        trace = jnp.sum(diag, axis=1, keepdims=True)
        traces.append(trace)
        innovs.append(full[128:129])
        y_ref[b] = a_mat / trace
        z_ref[b] = eye

    def step(i, carry):
        for b in range(NB):
            ys, zs = split3(y_ref[b]), split3(z_ref[b])
            u_mat = 0.5 * (3.0 * eye - mm(lhs_of(zs), rhs_of(ys)))
            us = split3(u_mat)
            y_ref[b] = mm(lhs_of(ys), rhs_of(us))
            z_ref[b] = mm(lhs_of(us), rhs_of(zs))
        return carry

    lax.fori_loop(0, NS_STEPS, step, 0)

    for b in range(NB):
        root = z_ref[b] / jnp.sqrt(traces[b])
        parts = split3(root)
        p_ana = mm(lhs_of(parts), rhs_of(parts))
        wbar = jnp.sum(p_ana * innovs[b], axis=1, keepdims=True)
        t_full = math.sqrt(MEM - 1.0) * root + wbar
        col_sum = jnp.sum(t_full, axis=0, keepdims=True)
        t_full = t_full + (1.0 - col_sum) * (1.0 / MEM)
        t1, t2, t3 = split3(t_full)
        t_ref[b] = jnp.concatenate([
            jnp.concatenate([t1, t3], axis=1),
            jnp.concatenate([t2, jnp.zeros_like(t2)], axis=1)], axis=0)

    for g in range(2):
        def apply(xb, carry, g=g):
            field = xt_ref[g * 16 + xb]
            out = jnp.dot(jnp.concatenate([field, field], axis=1), t_ref[lax.rem(xb, NB)], preferred_element_type=F32)
            u_ref[xb] = out[:, :128] + out[:, 128:]
            return carry
        lax.fori_loop(0, 16, apply, 0)

        def turn(c, carry, g=g):
            row = pl.multiple_of(c * 8, 8)
            tile = jnp.concatenate([u_ref[xb, pl.ds(row, 8), :] for xb in range(16)], axis=0)
            back = tile.T.astype(BF16)
            for d in range(8):
                o_ref[d, g, c, :, :] = back[16 * d:16 * d + 16]
            return carry
        lax.fori_loop(0, CH, turn, 0)


def update(g_left, g_right, g_west, g_east, xt):
    vm = pl.BlockSpec(memory_space=pltpu.VMEM)
    return pl.pallas_call(
        update_kernel,
        in_specs=[vm] * 5,
        out_specs=vm,
        out_shape=jax.ShapeDtypeStruct((8, 2, CH, 16, 128), BF16),
        scratch_shapes=[
            pltpu.VMEM((NB, 128, 128), F32),
            pltpu.VMEM((NB, 128, 128), F32),
            pltpu.VMEM((NB, 256, 256), BF16),
            pltpu.VMEM((16, KP, 128), F32),
        ],
        cost_estimate=pl.CostEstimate(flops=12_000_000_000, bytes_accessed=10_000_000, transcendentals=0),
        name="update",
        interpret=INTERPRET,
    )(g_left, g_right, g_west, g_east, xt)


def place_kernel(x_ref, *refs):
    o_ref, s_ref = refs[-2:]
    lane = lax.broadcasted_iota(jnp.int32, (16, 128), 1)

    def body(c, carry):
        for l in range(2):
            for g in range(2):
                tiles = [x_ref[4 * l + j, g, c, :, :].astype(F32) for j in range(4)]
                for xi, tile in enumerate(lane_swap(tiles, lane)):
                    row = COLS[g][xi] * PITCH
                    s_ref[l, row:row + 16, :] = tile
            for m in range(MLOC):
                o_ref[m, c, :, 128 * l:128 * l + 128] = s_ref.at[l][pl.ds(m, 8, stride=PITCH), :].astype(BF16)
        return carry
    lax.fori_loop(0, CH, body, 0)


def place(arrived, q, state):
    vm = pl.BlockSpec(memory_space=pltpu.VMEM)
    args, specs, alias = [arrived], [vm], {}
    if state is not None:
        args.append(state)
        specs.append(pl.BlockSpec(memory_space=pl.ANY))
        alias = {1: 0}
    return pl.pallas_call(
        place_kernel,
        grid=(1,),
        in_specs=[pl.BlockSpec((8, 2, CH, 16, 128), lambda i: (0, 0, 0, 0, 0))] + specs[1:],
        out_specs=pl.BlockSpec((MLOC, CH, LON, LATC), lambda i: (0, 0, 0, q)),
        out_shape=jax.ShapeDtypeStruct((MLOC, CH, LON, LATC * NCHUNK), BF16),
        scratch_shapes=[pltpu.VMEM((2, 8 * PITCH, 128), F32)],
        input_output_aliases=alias,
        cost_estimate=pl.CostEstimate(flops=4_000_000_000, bytes_accessed=10_000_000, transcendentals=0),
        name="place",
        interpret=INTERPRET,
    )(*args)


def shift(block, n_dom, offset):
    return lax.ppermute(block, 'dom', perm=[(s, (s + offset) % n_dom) for s in range(n_dom)])


def obs_rows(obs, me):
    mine = lax.dynamic_index_in_dim(obs.reshape(NCHUNK, 8, NB, PATCH, LON, OBS), me, axis=1, keepdims=False)
    order = COLS[0] + COLS[1]
    mine = jnp.stack([mine[:, :, :, x, :] for x in order], axis=1)
    return jnp.swapaxes(mine, 3, 4).reshape(NCHUNK, 8 * NB, OBS * PATCH)


def weights(w_in, w_out, obs_op):
    z = jnp.zeros((HID, CP - CH), BF16)
    w1t = jnp.concatenate([w_in[:CH].T, z, w_in[CH:].T, z], axis=1)
    w2t = jnp.concatenate([w_out.T, jnp.zeros((CP - CH, HID), BF16)], axis=0)
    hk = jnp.einsum('co,yz->oycz', obs_op, jnp.eye(PATCH, dtype=BF16)).reshape(OBS * PATCH, CH * PATCH)
    hk = jnp.concatenate([hk, jnp.zeros((OBS * PATCH, KP - CH * PATCH), BF16)], axis=1)
    return w1t, w2t, hk


def solution(mesh):
    n_dom = mesh.shape['dom']

    def exchange(block):
        return lax.all_to_all(block, 'ens', 0, 0, tiled=True)

    def local_cycle(ensemble, w_in, w_out, obs_op, obs_val, obs_wt):
        me = lax.axis_index('ens')
        xt = jnp.transpose(ensemble, (0, 3, 2, 1))
        w1t, w2t, hk = weights(w_in, w_out, obs_op)
        yo, wt = obs_rows(obs_val, me), obs_rows(obs_wt, me)

        arrived = []
        for q in range(NCHUNK):
            to_west, to_east = edge_columns(xt, q)
            halos = (shift(to_east, n_dom, 1), shift(to_west, n_dom, -1))
            if q == 0:
                arrived.append([exchange(forecast(xt, q, (g,), halos, w1t, w2t)) for g in (0, 1)])
            else:
                arrived.append([exchange(forecast(xt, q, (0, 1), halos, w1t, w2t))])

        state = None
        for q in range(NCHUNK):
            turned, g_left, g_right = gram(arrived[q], hk, yo[q], wt[q])
            g_west, g_east = shift(g_right, n_dom, 1), shift(g_left, n_dom, -1)
            back = exchange(update(g_left, g_right, g_west, g_east, turned))
            state = place(back, q, state)
        return jnp.transpose(state, (0, 3, 2, 1))

    state_spec = P('ens', None, 'dom', None)
    obs_spec = P(None, 'dom', None)
    return jax.shard_map(local_cycle, mesh=mesh, in_specs=(state_spec, P(), P(), P(), obs_spec, obs_spec),
                         out_specs=state_spec, check_vma=False)
```
